32 devices in a mesh: groups: 2 (over y), sp: 4 (over z), tp: 2 (over x), dp: 2 (over core).
Axes of the slice: x: 2, y: 2, z: 4, core: 2. Of those that a mesh axis runs over, the one named last changes fastest.
Arguments:
- queries: bfloat16 [4096, 4096], P(('groups', 'tp', 'dp', 'sp')), parts along dimension 0, may hold values from -6 to 6
- keys: bfloat16 [4096, 512], P(('groups', 'tp', 'dp', 'sp')), parts along dimension 0, may hold values from -6 to 6
- values: bfloat16 [4096, 512], P(('groups', 'tp', 'dp', 'sp')), parts along dimension 0, may hold values from -6 to 6
- doc_lengths: int32 [32], P('groups'), parts along dimension 0, may hold values from 1 to 256, 2048 in all
Outputs:
- attended: bfloat16 [4096, 4096], P(('groups', 'tp', 'dp', 'sp')), parts along dimension 0
The draws below stay inside these ranges and needn't reach their ends.
There are 2 independent parts, one for each index of `groups`. The reference program is written for one: setup_inputs(seed, part) draws one part's arguments, and reference() takes and returns one part's arrays. A program takes and returns all parts, laid end to end along the dimension named above; each array names one. Nothing has to cross between parts.
Inputs may be any that keep to these rules, and one draw needn't show every extreme that they name: `doc_lengths`: 16 documents whose lengths sum to 2048; the longest has exactly 256 tokens.
All inputs are finite; a program needn't handle non-finite values.
Results may differ from the reference program's by a relative error of at most 0.0038.
Values may be sent and summed in bfloat16 or wider, within the bound.
A program may use at most 64 MiB of HBM per device.

```python
import math
import jax
import jax.numpy as jnp
import numpy as np
from jax import lax

QUERY_HEADS = 32
KEY_VALUE_HEADS = 4
HEAD_SIZE = 128
SEQUENCE_TOKENS = 2048
LONGEST_DOCUMENT = 256
NDOC = 16


def draw_keys(key, part):
    attention_output = jnp.clip(jax.random.normal(jax.random.fold_in(key, 11), (SEQUENCE_TOKENS, KEY_VALUE_HEADS * HEAD_SIZE), jnp.float32), -6.0, 6.0)
    return attention_output.astype(jnp.bfloat16)


def draw_queries(key, part):
    attention_output = jnp.clip(jax.random.normal(jax.random.fold_in(key, 13), (SEQUENCE_TOKENS, QUERY_HEADS * HEAD_SIZE), jnp.float32), -6.0, 6.0)
    return attention_output.astype(jnp.bfloat16)


def block_levels(key, shape, pieces, smallest, top_value):
    level = 1.0
    for position, parts in pieces:
        heights = jax.random.uniform(jax.random.fold_in(jax.random.fold_in(key, 6), position), (parts,), jnp.float32, smallest / len(pieces), top_value / len(pieces))
        level = level * jnp.repeat(jnp.exp(heights), shape[position] // parts).reshape((-1,) + (1,) * (len(shape) - 1 - position))
    return level


def profile(amount, total, most, slope):
    loads = [(1 << 20) // math.isqrt(grade ** slope) + 1 for grade in range(2, amount + 1)]
    rest, given = total - most - (amount - 1), [1] * (amount - 1)
    while rest > 0:
        free = [i for i in range(amount - 1) if given[i] < most]
        whole, left = sum([loads[i] for i in free]), rest
        for i in free:
            extra = min(most - given[i], max(1, left * loads[i] // whole), rest)
            given[i] = given[i] + extra
            rest = rest - extra
    return np.array([most] + given)


def uneven(key, count, total, most, slope):
    if count == 2:
        one = jax.random.randint(key, (), max(1, total - most), min(most, total - 1) + 1)
        return jnp.stack([one, total - one])
    tallies = jnp.asarray(profile(count, total, most, slope), jnp.int32)
    couples = (count - 1) // 2
    source_of, sink = tallies[1:1 + 2 * couples:2], tallies[2:2 + 2 * couples:2]
    margin = jnp.minimum(source_of - 1, most - sink)
    moved = jax.random.randint(jax.random.fold_in(key, 1), (couples,), 0, 1 << 20) % (margin + 1)
    tallies = tallies.at[1:1 + 2 * couples:2].set(source_of - moved).at[2:2 + 2 * couples:2].set(sink + moved)
    return tallies[jax.random.permutation(jax.random.fold_in(key, 2), count)]


def centred(stream_key, extent, spread, bound, shards=(), kind=jnp.bfloat16):
    array = jax.random.normal(stream_key, extent, jnp.float32) * spread
    if len(shards) > 0:
        array = block_levels(stream_key, extent, shards, -0.22, 0.18) * array
    return jnp.clip(array, min=-bound, max=bound).astype(kind)


def setup_inputs(seed: int = 0, part: int = 0) -> dict:
    key_list = jax.random.split(jax.random.key(seed), 5)
    part_splits = jax.random.split(jax.random.fold_in(key_list[4], part), 5)
    return {
        "queries": draw_queries(jax.random.fold_in(jax.random.fold_in(key_list[4], part), 71), part),
        "keys": draw_keys(jax.random.fold_in(jax.random.fold_in(key_list[4], part), 71), part),
        "values": centred(part_splits[2], (SEQUENCE_TOKENS, KEY_VALUE_HEADS * HEAD_SIZE), 1.0, 6.0, ((0, 16),)),
        "doc_lengths": uneven(part_splits[3], NDOC, SEQUENCE_TOKENS, LONGEST_DOCUMENT, 2).astype(jnp.int32),
    }


def reference(queries, keys, values, doc_lengths):
    ends = jnp.cumsum(doc_lengths).astype(jnp.int32)
    positions = jnp.arange(SEQUENCE_TOKENS, dtype=jnp.int32)
    doc = jnp.sum((positions[:, None] >= ends[None, :]).astype(jnp.int32), axis=1)
    query_group = QUERY_HEADS // KEY_VALUE_HEADS
    block = math.gcd(LONGEST_DOCUMENT, 512)
    blocks = SEQUENCE_TOKENS // block
    reach = LONGEST_DOCUMENT + block
    q_heads = queries.reshape(SEQUENCE_TOKENS, QUERY_HEADS, HEAD_SIZE).transpose(1, 0, 2)
    leading_part = jnp.zeros((LONGEST_DOCUMENT, KEY_VALUE_HEADS * HEAD_SIZE), jnp.bfloat16)
    key_head_rows = jnp.concatenate([leading_part, keys], axis=0).reshape(SEQUENCE_TOKENS + LONGEST_DOCUMENT, KEY_VALUE_HEADS, HEAD_SIZE).transpose(1, 0, 2)
    value_head_rows = jnp.concatenate([leading_part, values], axis=0).reshape(SEQUENCE_TOKENS + LONGEST_DOCUMENT, KEY_VALUE_HEADS, HEAD_SIZE).transpose(1, 0, 2)
    pad_pos = jnp.arange(SEQUENCE_TOKENS + LONGEST_DOCUMENT, dtype=jnp.int32) - LONGEST_DOCUMENT
    pad_doc = jnp.concatenate([jnp.full((LONGEST_DOCUMENT,), -1, jnp.int32), doc.astype(jnp.int32)], axis=0)
    scale = HEAD_SIZE ** -0.5

    def one_head(head):
        q_all = lax.dynamic_index_in_dim(q_heads, head, 0, keepdims=False)
        k_all = lax.dynamic_index_in_dim(key_head_rows, head // query_group, 0, keepdims=False)
        v_all = lax.dynamic_index_in_dim(value_head_rows, head // query_group, 0, keepdims=False)

        def one_block(index):
            first = (index * block).astype(jnp.int32)
            q_rows = lax.dynamic_slice_in_dim(q_all, first, block, 0)
            q_pos = first + jnp.arange(block, dtype=jnp.int32)
            q_doc = lax.dynamic_slice_in_dim(doc, first, block, 0)
            k_rows = lax.dynamic_slice_in_dim(k_all, first, reach, 0)
            v_rows = lax.dynamic_slice_in_dim(v_all, first, reach, 0)
            k_pos = lax.dynamic_slice_in_dim(pad_pos, first, reach, 0)
            k_doc = lax.dynamic_slice_in_dim(pad_doc, first, reach, 0)
            score = jnp.dot(q_rows, k_rows.T, preferred_element_type=jnp.float32) * scale
            live = (k_pos[None, :] <= q_pos[:, None]) & (k_doc[None, :] == q_doc[:, None])
            top = jnp.max(jnp.where(live, score, -jnp.inf), axis=1)
            weight = jnp.where(live, jnp.exp(score - top[:, None]), 0.0)
            total = jnp.sum(weight, axis=1)
            summed = jnp.dot(weight.astype(jnp.bfloat16), v_rows, preferred_element_type=jnp.float32)
            return (summed / total[:, None]).astype(jnp.bfloat16)

        return lax.map(one_block, jnp.arange(blocks, dtype=jnp.int32)).reshape(SEQUENCE_TOKENS, HEAD_SIZE)

    attention_output = lax.map(one_head, jnp.arange(QUERY_HEADS, dtype=jnp.int32))
    return attention_output.transpose(1, 0, 2).reshape(SEQUENCE_TOKENS, QUERY_HEADS * HEAD_SIZE)
```

```python
import functools
import math

import jax
import jax.numpy as jnp
from jax import lax
from jax.experimental import pallas as pl
from jax.experimental.pallas import tpu as pltpu
from jax.sharding import PartitionSpec as P

HEAD_SIZE = 128
MESH = pl.DeviceIdType.MESH
DEAD = -1e30


def place(index, dp_count, sp_count):
    return {
        "tp": index // (dp_count * sp_count),
        "dp": (index // sp_count) % dp_count,
        "sp": index % sp_count,
    }


def kernel(
    sizes, q_hbm, k_hbm, v_hbm, lengths_hbm, out_buf,
    q_buf, held, bias, lengths, q_sem, kv_sem, send_sem, recv_sem, lengths_sem,
):
    tp_count, dp_count, sp_count, hops, heads, group = sizes
    rows = q_hbm.shape[0]
    width = group * HEAD_SIZE
    blocks = tp_count * dp_count * sp_count
    me = (lax.axis_index("tp") * dp_count + lax.axis_index("dp")) * sp_count + lax.axis_index("sp")
    right = place(lax.rem(me + 1, blocks), dp_count, sp_count)
    left = place(lax.rem(me + blocks - 1, blocks), dp_count, sp_count)

    def load(source, which, head):
        columns = pl.ds(head * HEAD_SIZE, HEAD_SIZE)
        return pltpu.make_async_copy(
            source.at[:, columns], held.at[0, head, which], kv_sem.at[head, which]
        )

    def load_q(head):
        columns = pl.ds(head * width, width)
        return pltpu.make_async_copy(q_hbm.at[:, columns], q_buf.at[:, columns], q_sem.at[head])

    def send(hop, head):
        return pltpu.make_async_remote_copy(
            src_ref=held.at[hop, head],
            dst_ref=held.at[hop + 1, head],
            send_sem=send_sem.at[hop, head],
            recv_sem=recv_sem.at[hop, head],
            device_id=right,
            device_id_type=MESH,
        )

    def start_send(hop, head):
        @pl.when((me >= hop) & (me < blocks - 1))
        def _():
            send(hop, head).start()

    def wait_receive(hop, head):
        @pl.when(me >= hop)
        def _():
            send(hop - 1, head).wait_recv()

    get_lengths = pltpu.make_async_copy(lengths_hbm, lengths, lengths_sem)
    for head in range(heads):
        load(k_hbm, 0, head).start()
        load(v_hbm, 1, head).start()
    for head in range(heads):
        load_q(head).start()
    get_lengths.start()

    barrier = pltpu.get_barrier_semaphore()

    @pl.when(me > 0)
    def _():
        pl.semaphore_signal(barrier, inc=1, device_id=left, device_id_type=MESH)

    @pl.when(me < blocks - 1)
    def _():
        pl.semaphore_wait(barrier, 1)

    for head in range(heads):
        load(k_hbm, 0, head).wait()
        load(v_hbm, 1, head).wait()
        start_send(0, head)
    for hop in range(1, hops + 1):

        @pl.when(me < hop)
        def _():
            held[hop] = jnp.zeros_like(held[hop])

    get_lengths.wait()
    base = me * rows
    row = lax.broadcasted_iota(jnp.int32, (rows, rows), 0)
    column = lax.broadcasted_iota(jnp.int32, (rows, rows), 1)
    near = column <= row
    first = jnp.zeros((rows, rows), jnp.int32)
    end = jnp.int32(0)
    for entry in range(lengths.shape[0]):
        end = end + lengths[entry]
        first = jnp.where(base + row >= end, end, first)
    mixed_position = base + column - jnp.where(near, 0, hops * rows)
    bias[0] = jnp.where(mixed_position >= first, 0.0, DEAD)
    for hop in range(1, hops):
        bias[hop] = jnp.where(base - hop * rows + column >= first, 0.0, DEAD)

    for hop in range(1, hops):
        for head in range(heads):
            wait_receive(hop, head)
            start_send(hop, head)

    factor = HEAD_SIZE ** (-0.5) * math.log2(math.e)
    span = (hops + 1) * rows
    batch = math.gcd(group, 8)
    for head in range(heads):
        wait_receive(hops, head)
        load_q(head).wait()
        k_all = held[:, head, 0].reshape(span, HEAD_SIZE)
        v_all = held[:, head, 1].reshape(span, HEAD_SIZE)
        for member in range(0, group, batch):
            at = [head * width + (member + other) * HEAD_SIZE for other in range(batch)]
            q_rows = jnp.concatenate([q_buf[:, a : a + HEAD_SIZE] for a in at], axis=0)
            score = lax.dot_general(
                q_rows, k_all, (((1,), (1,)), ((), ())), preferred_element_type=jnp.float32
            ).reshape(batch, rows, span)
            parts = [score[:, :, hop * rows : (hop + 1) * rows] for hop in range(hops + 1)]
            mixed = jnp.where(near, parts[0], parts[hops])
            parts = [part + bias[hop] for hop, part in enumerate([mixed] + parts[1:hops])]
            top = jnp.max(functools.reduce(jnp.maximum, parts), axis=2, keepdims=True)
            weights = [jnp.exp2((part - top) * factor) for part in parts]
            total = jnp.sum(sum(weights[1:], weights[0]), axis=2, keepdims=True)
            ends = [jnp.where(near, weights[0], 0.0), jnp.where(near, 0.0, weights[0])]
            weight = jnp.concatenate([ends[0]] + weights[1:] + [ends[1]], axis=2)
            weight = weight.astype(jnp.bfloat16).reshape(batch * rows, span)
            summed = jnp.dot(weight, v_all, preferred_element_type=jnp.float32)
            result = (summed.reshape(batch, rows, HEAD_SIZE) / total).astype(jnp.bfloat16)
            for other, a in enumerate(at):
                out_buf[:, a : a + HEAD_SIZE] = result[other]

    for hop in range(hops):
        for head in range(heads):

            @pl.when((me >= hop) & (me < blocks - 1))
            def _():
                send(hop, head).wait_send()


def solution(mesh):
    tp_count, dp_count, sp_count = (mesh.shape[axis] for axis in ("tp", "dp", "sp"))
    hops = max(sp_count // 2, 1)

    def local(queries, keys, values, doc_lengths):
        rows, width = queries.shape
        heads = keys.shape[1] // HEAD_SIZE
        group = width // keys.shape[1]
        sizes = (tp_count, dp_count, sp_count, hops, heads, group)
        hbm = pl.BlockSpec(memory_space=pltpu.HBM)
        return pl.pallas_call(
            functools.partial(kernel, sizes),
            out_shape=jax.ShapeDtypeStruct((rows, width), jnp.bfloat16),
            in_specs=[hbm, hbm, hbm, hbm],
            out_specs=pl.BlockSpec(memory_space=pltpu.VMEM),
            scratch_shapes=[
                pltpu.VMEM((rows, width), jnp.bfloat16),
                pltpu.VMEM((hops + 1, heads, 2, rows, HEAD_SIZE), jnp.bfloat16),
                pltpu.VMEM((hops, rows, rows), jnp.float32),
                pltpu.SMEM(doc_lengths.shape, jnp.int32),
                pltpu.SemaphoreType.DMA((heads,)),
                pltpu.SemaphoreType.DMA((heads, 2)),
                pltpu.SemaphoreType.DMA((hops, heads)),
                pltpu.SemaphoreType.DMA((hops, heads)),
                pltpu.SemaphoreType.DMA,
            ],
            compiler_params=pltpu.CompilerParams(collective_id=0, has_side_effects=True, vmem_limit_bytes=32 << 20),
        )(*(pltpu.with_memory_space_constraint(x, pltpu.HBM) for x in (queries, keys, values, doc_lengths)))

    spec = P(("groups", "tp", "dp", "sp"), None)
    return jax.shard_map(
        local, mesh=mesh, in_specs=(spec, spec, spec, P("groups")), out_specs=spec, check_vma=False
    )
```

```python
import functools
import math

import jax
import jax.numpy as jnp
from jax import lax
from jax.experimental import pallas as pl
from jax.experimental.pallas import tpu as pltpu
from jax.sharding import PartitionSpec as P

HEAD_SIZE = 128
MESH = pl.DeviceIdType.MESH
DEAD = -1e30


def kernel(
    sizes, q_hbm, k_hbm, v_hbm, lengths_hbm, out_buf,
    q_buf, held, stage, bias, top_buf, total_buf, summed_buf, lengths,
    q_sem, kv_sem, send_sem, far_sem, recv_sem, stage_sem, lengths_sem, ready_sem,
):
    tp_count, dp_count, sp_count, hops, heads, group = sizes
    rows = q_hbm.shape[0]
    lines = dp_count * sp_count
    blocks = tp_count * lines
    line, core, plane = (lax.axis_index(axis) for axis in ("sp", "dp", "tp"))
    me = (plane * dp_count + core) * sp_count + line

    def device(index):
        index = lax.rem(index + 2 * blocks, blocks)
        return {"tp": index // lines, "dp": (index // sp_count) % dp_count, "sp": index % sp_count}

    far = sp_count - line
    is_far = (far <= hops) & (me + far < blocks)
    crosses = core == dp_count - 1
    even = lax.rem(far, 2) == 0
    turns = is_far & crosses & even
    goes_far = is_far & jnp.logical_not(turns)
    relays = (far <= hops) & crosses & even & (plane >= 1)
    to_right = line < sp_count - 1
    right, left, turn, turned = device(me + 1), device(me - 1), device(me + lines), device(me - lines)
    far_target = device(me + far - jnp.where(relays, lines, 0))

    def far_sender(target, distance):
        return device(target - distance + (jnp.where(core == 0, lines, 0) if distance % 2 == 0 else 0))

    def load(head, which):
        source = (k_hbm, v_hbm)[which]
        return pltpu.make_async_copy(
            source.at[:, pl.ds(head * HEAD_SIZE, HEAD_SIZE)], held.at[0, head, which], kv_sem.at[head, which]
        )

    def load_q(head, member):
        return pltpu.make_async_copy(
            q_hbm.at[:, pl.ds((head * group + member) * HEAD_SIZE, HEAD_SIZE)],
            q_buf.at[head, pl.ds(member * rows, rows)],
            q_sem.at[head, member],
        )

    def copy(source, target, send, receive, where):
        return pltpu.make_async_remote_copy(
            src_ref=source, dst_ref=target, send_sem=send, recv_sem=receive, device_id=where, device_id_type=MESH
        )

    def forward(slot, head):
        return copy(
            held.at[slot, head], held.at[slot + 1, head], send_sem.at[slot, head], recv_sem.at[slot + 1, head], right
        )

    def send_far(head):
        return copy(held.at[0, head], held.at[far, head], far_sem.at[head], recv_sem.at[far, head], far_target)

    def send_turn(head):
        return copy(held.at[0, head], stage.at[head], far_sem.at[head], stage_sem.at[0, head], turn)

    def send_relay(head):
        return copy(stage.at[head], held.at[far, head], stage_sem.at[1, head], recv_sem.at[far, head], far_target)

    def receive(slot, head):
        pl.when(me >= slot)(forward(slot - 1, head).wait_recv)
        if slot < hops:
            pl.when(to_right & (me >= slot))(forward(slot, head).start)

    barrier = pltpu.get_barrier_semaphore()

    def greet(condition, where, semaphore=barrier):
        @pl.when(condition)
        def _():
            pl.semaphore_signal(semaphore, inc=1, device_id=where, device_id_type=MESH)

    def hear(condition):
        @pl.when(condition)
        def _():
            pl.semaphore_wait(ready_sem, 1)

    greet(line >= 1, left)
    greet((line == 0) & (me >= 1), far_sender(me, 1))
    greet(relays, turned)
    if hops > 1:
        greet((line == 0) & (me >= 2), right)
        greet((goes_far & to_right) | relays, device(me + far - jnp.where(relays, lines, 0) + 1))
    get_lengths = pltpu.make_async_copy(lengths_hbm, lengths, lengths_sem)
    for head in range(heads):
        for which in range(2):
            load(head, which).start()
    get_lengths.start()
    for head in range(heads):
        for member in range(group):
            load_q(head, member).start()
    meets = [to_right, goes_far & jnp.logical_not(to_right), turns]
    if hops > 1:
        introduced = [(line == 1) & (me > distance) for distance in range(2, hops + 1)]
        meets += [(line == 1) & (me >= 3)] + introduced
    peers = sum(condition.astype(jnp.int32) for condition in meets)

    @pl.when(peers > 0)
    def _():
        pl.semaphore_wait(barrier, peers)

    if hops > 1:
        for distance, condition in enumerate(introduced, 2):
            greet(condition, far_sender(me - 1, distance), ready_sem)
    for head in range(heads):
        for which in range(2):
            load(head, which).wait()
        pl.when(to_right)(forward(0, head).start)
        pl.when(goes_far & jnp.logical_not(to_right))(send_far(head).start)
        pl.when(turns)(send_turn(head).start)
    for slot in range(1, hops + 1):

        @pl.when(me < slot)
        def _():
            held[slot] = jnp.zeros_like(held[slot])

    get_lengths.wait()
    base = me * rows
    row = lax.broadcasted_iota(jnp.int32, (rows, rows), 0)
    column = lax.broadcasted_iota(jnp.int32, (rows, rows), 1)
    first = jnp.zeros((rows, rows), jnp.int32)
    end = jnp.int32(0)
    for entry in range(lengths.shape[0]):
        end = end + lengths[entry]
        first = jnp.where(base + row >= end, end, first)
    bias[0] = jnp.where((column <= row) & (base + column >= first), 0.0, DEAD)
    for slot in range(1, hops + 1):
        bias[slot] = jnp.where(base - slot * rows + column >= first, 0.0, DEAD)

    factor = HEAD_SIZE ** (-0.5) * math.log2(math.e)

    def weigh(step, slot, head):
        score = lax.dot_general(
            q_buf[head], held[slot, head, 0], (((1,), (1,)), ((), ())), preferred_element_type=jnp.float32
        )
        score = score.reshape(group, rows, rows) + bias[slot]
        top = jnp.max(score, axis=2, keepdims=True)
        fade = None
        if step > 0:
            before = top_buf[head].reshape(group, rows, HEAD_SIZE)
            top = jnp.maximum(top, before)
            fade = jnp.exp2((before - top) * factor)
        weight = jnp.exp2((score - top) * factor)
        total = jnp.sum(weight, axis=2, keepdims=True)
        if step > 0:
            total = total + total_buf[head].reshape(group, rows, HEAD_SIZE) * fade
        return weight.astype(jnp.bfloat16).reshape(group * rows, rows), top, total, fade

    def flat(x):
        return jnp.broadcast_to(x, (group, rows, HEAD_SIZE)).reshape(group * rows, HEAD_SIZE)

    for step in range(hops + 1):
        for head in range(heads):
            if step == 0:
                for member in range(group):
                    load_q(head, member).wait()
            else:
                if step == 1:
                    if head == 0:
                        hear(relays)

                    @pl.when(relays)
                    def _():
                        send_turn(head).wait_recv()
                        send_relay(head).start()

                receive(step, head)
            weight, top, total, fade = weigh(step, step, head)
            summed = jnp.dot(weight, held[step, head, 1], preferred_element_type=jnp.float32)
            if step < hops:
                top_buf[head] = flat(top)
                total_buf[head] = flat(total)
                summed_buf[head] = summed if step == 0 else summed_buf[head] * flat(fade) + summed
            else:
                inverse = 1.0 / flat(total)
                kept = summed_buf[head] * (flat(fade) * inverse)
                result = (kept + summed * inverse).astype(jnp.bfloat16)
                for member in range(group):
                    a = (head * group + member) * HEAD_SIZE
                    out_buf[:, a : a + HEAD_SIZE] = result[member * rows : (member + 1) * rows]

        if step == 0:
            hear(goes_far & to_right)

            @pl.when(goes_far & to_right)
            def _():
                for head in range(heads):
                    send_far(head).start()

    for head in range(heads):
        pl.when(to_right)(forward(0, head).wait_send)
        pl.when(goes_far)(send_far(head).wait_send)
        pl.when(turns)(send_turn(head).wait_send)
        pl.when(relays)(send_relay(head).wait_send)
        for slot in range(1, hops):
            pl.when(to_right & (me >= slot))(forward(slot, head).wait_send)


def solution(mesh):
    tp_count, dp_count, sp_count = (mesh.shape[axis] for axis in ("tp", "dp", "sp"))
    hops = max(sp_count // 2, 1)

    def local(queries, keys, values, doc_lengths):
        rows, width = queries.shape
        heads = keys.shape[1] // HEAD_SIZE
        group = width // keys.shape[1]
        sizes = (tp_count, dp_count, sp_count, hops, heads, group)
        hbm = pl.BlockSpec(memory_space=pltpu.HBM)
        arguments = (queries, keys, values, doc_lengths)
        return pl.pallas_call(
            functools.partial(kernel, sizes),
            out_shape=jax.ShapeDtypeStruct((rows, width), jnp.bfloat16),
            in_specs=[hbm, hbm, hbm, hbm],
            out_specs=pl.BlockSpec(memory_space=pltpu.VMEM),
            scratch_shapes=[
                pltpu.VMEM((heads, group * rows, HEAD_SIZE), jnp.bfloat16),
                pltpu.VMEM((hops + 1, heads, 2, rows, HEAD_SIZE), jnp.bfloat16),
                pltpu.VMEM((heads, 2, rows, HEAD_SIZE), jnp.bfloat16),
                pltpu.VMEM((hops + 1, rows, rows), jnp.float32),
                pltpu.VMEM((heads, group * rows, HEAD_SIZE), jnp.float32),
                pltpu.VMEM((heads, group * rows, HEAD_SIZE), jnp.float32),
                pltpu.VMEM((heads, group * rows, HEAD_SIZE), jnp.float32),
                pltpu.SMEM(doc_lengths.shape, jnp.int32),
                pltpu.SemaphoreType.DMA((heads, group)),
                pltpu.SemaphoreType.DMA((heads, 2)),
                pltpu.SemaphoreType.DMA((hops, heads)),
                pltpu.SemaphoreType.DMA((heads,)),
                pltpu.SemaphoreType.DMA((hops + 1, heads)),
                pltpu.SemaphoreType.DMA((2, heads)),
                pltpu.SemaphoreType.DMA,
                pltpu.SemaphoreType.REGULAR,
            ],
            compiler_params=pltpu.CompilerParams(collective_id=0, has_side_effects=True, vmem_limit_bytes=40 << 20),
        )(*(pltpu.with_memory_space_constraint(x, pltpu.HBM) for x in arguments))

    spec = P(("groups", "tp", "dp", "sp"), None)
    return jax.shard_map(
        local, mesh=mesh, in_specs=(spec, spec, spec, P("groups")), out_specs=spec, check_vma=False
    )
```

```python
import functools
import math

import jax
import jax.numpy as jnp
from jax import lax
from jax.experimental import pallas as pl
from jax.experimental.pallas import tpu as pltpu
from jax.sharding import PartitionSpec as P

HEAD_SIZE = 128
MESH = pl.DeviceIdType.MESH
DEAD = -1e30


def kernel(
    sizes, q_hbm, k_hbm, v_hbm, lengths_hbm, out_buf,
    q_buf, held, stage, bias, top_buf, total_buf, summed_buf, lengths,
    q_sem, kv_sem, send_sem, far_sem, recv_sem, stage_sem, lengths_sem,
):
    tp_count, dp_count, sp_count, hops, heads, group = sizes
    rows = q_hbm.shape[0]
    lines = dp_count * sp_count
    blocks = tp_count * lines
    line, core, plane = (lax.axis_index(axis) for axis in ("sp", "dp", "tp"))
    me = (plane * dp_count + core) * sp_count + line

    def device(index):
        index = lax.rem(index + 2 * blocks, blocks)
        return {"tp": index // lines, "dp": (index // sp_count) % dp_count, "sp": index % sp_count}

    far = sp_count - line
    is_far = (far <= hops) & (me + far < blocks)
    crosses = core == dp_count - 1
    odd = lax.rem(far, 2) == 1
    turns = is_far & crosses & odd
    goes_far = is_far & jnp.logical_not(turns)
    relays = (far <= hops) & crosses & odd & (plane >= 1)
    to_right = line < sp_count - 1
    right, left, turn, turned = device(me + 1), device(me - 1), device(me + lines), device(me - lines)
    far_target = device(me + far - jnp.where(relays, lines, 0))

    def far_sender(target, distance):
        return device(target - distance + (jnp.where(core == 0, lines, 0) if distance % 2 == 1 else 0))

    def load(head, which):
        source = (k_hbm, v_hbm)[which]
        return pltpu.make_async_copy(
            source.at[:, pl.ds(head * HEAD_SIZE, HEAD_SIZE)], held.at[0, 2 * head + which], kv_sem.at[head]
        )

    get_q = pltpu.make_async_copy(q_hbm, q_buf, q_sem)

    def copy(source, target, send, receive, where):
        return pltpu.make_async_remote_copy(
            src_ref=source, dst_ref=target, send_sem=send, recv_sem=receive, device_id=where, device_id_type=MESH
        )

    pieces = [pl.ds(2 * head, 2) for head in range(heads)]

    def new_pieces(row, count=1):
        return [n for n, piece in enumerate(pieces) if row <= piece.start < row + count]

    def forward(slot, n):
        rows_of = pieces[n]
        return copy(
            held.at[slot, rows_of], held.at[slot + 1, rows_of], send_sem, recv_sem.at[slot, n], right
        )

    def send_far(n):
        rows_of = pieces[n]
        return copy(held.at[0, rows_of], held.at[far, rows_of], far_sem, recv_sem.at[far - 1, n], far_target)

    def send_turn(n):
        rows_of = pieces[n]
        return copy(held.at[0, rows_of], stage.at[rows_of], far_sem, stage_sem.at[n], turn)

    def send_relay(n):
        rows_of = pieces[n]
        return copy(stage.at[rows_of], held.at[far, rows_of], far_sem, recv_sem.at[far - 1, n], far_target)

    def receive(slot, n):
        pl.when(me >= slot)(forward(slot - 1, n).wait_recv)
        if slot < hops:
            pl.when(to_right & (me >= slot))(forward(slot, n).start)

    barrier = pltpu.get_barrier_semaphore()

    def greet(condition, where):
        @pl.when(condition)
        def _():
            pl.semaphore_signal(barrier, inc=1, device_id=where, device_id_type=MESH)

    greet(line >= 1, left)
    for distance in range(1, hops + 1):
        greet((line == 0) & (me >= distance), far_sender(me, distance))
    greet(relays, turned)
    get_lengths = pltpu.make_async_copy(lengths_hbm, lengths, lengths_sem)
    for head in range(heads):
        for which in range(2):
            load(head, which).start()
    peers = sum(condition.astype(jnp.int32) for condition in (to_right, goes_far, relays, turns))

    @pl.when(peers > 0)
    def _():
        pl.semaphore_wait(barrier, peers)

    for n, piece in enumerate(pieces):
        for head in range(piece.start // 2, (piece.start + piece.size) // 2):
            both = held.at[0, pl.ds(2 * head, 2)]
            pltpu.make_async_copy(both, both, kv_sem.at[head]).wait()
        pl.when(to_right)(forward(0, n).start)
        pl.when(turns)(send_turn(n).start)
        pl.when(goes_far & jnp.logical_not(to_right))(send_far(n).start)
    get_lengths.start()
    get_q.start()
    for slot in range(1, hops + 1):

        @pl.when(me < slot)
        def _():
            held[slot] = jnp.zeros_like(held[slot])

    get_lengths.wait()
    base = me * rows
    row = lax.broadcasted_iota(jnp.int32, (rows, rows), 0)
    column = lax.broadcasted_iota(jnp.int32, (rows, rows), 1)
    first = jnp.zeros((rows, rows), jnp.int32)
    end = jnp.int32(0)
    for entry in range(lengths.shape[0]):
        end = end + lengths[entry]
        first = jnp.where(base + row >= end, end, first)
    bias[0] = jnp.where((column <= row) & (base + column >= first), 0.0, DEAD)
    for slot in range(1, hops + 1):
        bias[slot] = jnp.where(base - slot * rows + column >= first, 0.0, DEAD)

    factor = HEAD_SIZE ** (-0.5) * math.log2(math.e)

    def weigh(step, slot, head):
        columns = [(head * group + member) * HEAD_SIZE for member in range(group)]
        queries = jnp.concatenate([q_buf[:, a : a + HEAD_SIZE] for a in columns], axis=0)
        score = lax.dot_general(
            queries, held[slot, 2 * head], (((1,), (1,)), ((), ())), preferred_element_type=jnp.float32
        )
        score = score.reshape(group, rows, rows) + bias[slot]
        top = jnp.max(score, axis=2, keepdims=True)
        fade = None
        if step > 0:
            before = top_buf[head].reshape(group, rows, HEAD_SIZE)
            top = jnp.maximum(top, before)
            fade = jnp.exp2((before - top) * factor)
        weight = jnp.exp2((score - top) * factor)
        total = jnp.sum(weight, axis=2, keepdims=True)
        if step > 0:
            total = total + total_buf[head].reshape(group, rows, HEAD_SIZE) * fade
        return weight.astype(jnp.bfloat16).reshape(group * rows, rows), top, total, fade

    def flat(x):
        return jnp.broadcast_to(x, (group, rows, HEAD_SIZE)).reshape(group * rows, HEAD_SIZE)

    def start_far(condition):
        @pl.when(goes_far & to_right & condition)
        def _():
            for n in range(len(pieces)):
                send_far(n).start()

    start_far(jnp.logical_not(crosses))
    get_q.wait()
    for step in range(hops + 1):
        for head in range(heads):
            if step > 0:
                if step == 1:

                    @pl.when(relays)
                    def _():
                        for n in new_pieces(2 * head, 2):
                            send_turn(n).wait_recv()
                            send_relay(n).start()

                for n in new_pieces(2 * head):
                    receive(step, n)
            weight, top, total, fade = weigh(step, step, head)
            if step > 0:
                for n in new_pieces(2 * head + 1):
                    receive(step, n)
            summed = jnp.dot(weight, held[step, 2 * head + 1], preferred_element_type=jnp.float32)
            if step < hops:
                top_buf[head] = flat(top)
                total_buf[head] = flat(total)
                summed_buf[head] = summed if step == 0 else summed_buf[head] * flat(fade) + summed
            else:
                inverse = 1.0 / flat(total)
                kept = summed_buf[head] * (flat(fade) * inverse)
                result = (kept + summed * inverse).astype(jnp.bfloat16)
                for member in range(group):
                    a = (head * group + member) * HEAD_SIZE
                    out_buf[:, a : a + HEAD_SIZE] = result[member * rows : (member + 1) * rows]
            if step == 1 and head == heads // 2:
                start_far(crosses)

    def wait_sent(condition, count, sem):
        for slots in range(1, hops + 1):

            @pl.when(condition & (count == slots))
            def _():
                sent = held.at[pl.ds(0, slots)]
                pltpu.make_async_copy(sent, sent, sem).wait()

    wait_sent(to_right, jnp.minimum(me + 1, hops), send_sem)
    wait_sent(goes_far | turns | relays, (goes_far | turns).astype(jnp.int32) + relays.astype(jnp.int32), far_sem)


def solution(mesh):
    tp_count, dp_count, sp_count = (mesh.shape[axis] for axis in ("tp", "dp", "sp"))
    hops = max(sp_count // 2, 1)

    def local(queries, keys, values, doc_lengths):
        rows, width = queries.shape
        heads = keys.shape[1] // HEAD_SIZE
        group = width // keys.shape[1]
        sizes = (tp_count, dp_count, sp_count, hops, heads, group)
        hbm = pl.BlockSpec(memory_space=pltpu.HBM)
        arguments = (queries, keys, values, doc_lengths)
        return pl.pallas_call(
            functools.partial(kernel, sizes),
            out_shape=jax.ShapeDtypeStruct((rows, width), jnp.bfloat16),
            in_specs=[hbm, hbm, hbm, hbm],
            out_specs=pl.BlockSpec(memory_space=pltpu.VMEM),
            scratch_shapes=[
                pltpu.VMEM((rows, width), jnp.bfloat16),
                pltpu.VMEM((hops + 1, 2 * heads, rows, HEAD_SIZE), jnp.bfloat16),
                pltpu.VMEM((2 * heads, rows, HEAD_SIZE), jnp.bfloat16),
                pltpu.VMEM((hops + 1, rows, rows), jnp.float32),
                pltpu.VMEM((heads, group * rows, HEAD_SIZE), jnp.float32),
                pltpu.VMEM((heads, group * rows, HEAD_SIZE), jnp.float32),
                pltpu.VMEM((heads, group * rows, HEAD_SIZE), jnp.float32),
                pltpu.SMEM(doc_lengths.shape, jnp.int32),
                pltpu.SemaphoreType.DMA,
                pltpu.SemaphoreType.DMA((heads,)),
                pltpu.SemaphoreType.DMA,
                pltpu.SemaphoreType.DMA,
                pltpu.SemaphoreType.DMA((hops, heads)),
                pltpu.SemaphoreType.DMA((heads,)),
                pltpu.SemaphoreType.DMA,
            ],
            compiler_params=pltpu.CompilerParams(collective_id=0, has_side_effects=True, vmem_limit_bytes=40 << 20),
        )(*(pltpu.with_memory_space_constraint(x, pltpu.HBM) for x in arguments))

    spec = P(("groups", "tp", "dp", "sp"), None)
    return jax.shard_map(
        local, mesh=mesh, in_specs=(spec, spec, spec, P("groups")), out_specs=spec, check_vma=False
    )
```

```python
import functools
import math

import jax
import jax.numpy as jnp
from jax import lax
from jax.experimental import pallas as pl
from jax.experimental.pallas import tpu as pltpu
from jax.sharding import PartitionSpec as P

HEAD_SIZE = 128
MESH = pl.DeviceIdType.MESH
DEAD = -1e30


def queries_of(q_buf, head, group):
    columns = [(head * group + member) * HEAD_SIZE for member in range(group)]
    return jnp.concatenate([q_buf[:, a : a + HEAD_SIZE] for a in columns], axis=0)


def attend(queries, keys, values, bias, before):
    rows = keys.shape[0]
    factor = HEAD_SIZE ** (-0.5) * math.log2(math.e)
    score = lax.dot_general(queries, keys, (((1,), (1,)), ((), ())), preferred_element_type=jnp.float32)
    score = (score.reshape(-1, rows, rows) + bias).reshape(-1, rows)
    top = jnp.max(score, axis=1, keepdims=True)
    if before is not None:
        top_before, total_before, summed_before = before
        top = jnp.maximum(top, top_before)
        fade = jnp.exp2((top_before - top) * factor)
    weight = jnp.exp2((score - top) * factor)
    total = jnp.sum(weight, axis=1, keepdims=True)
    summed = jnp.dot(weight.astype(jnp.bfloat16), values, preferred_element_type=jnp.float32)
    if before is not None:
        total = total + total_before * fade
        summed = summed + summed_before * fade
    return jnp.broadcast_to(top, summed.shape), jnp.broadcast_to(total, summed.shape), summed


def finish(heads, group, done, q_buf, last_kv, last_bias, last_top, last_total, last_summed, out, result_buf, sem):
    rows = last_kv.shape[1]
    rest = (heads - 1) * group * HEAD_SIZE
    for head in range(heads - 1):
        columns = pl.ds(head * group * HEAD_SIZE, group * HEAD_SIZE)
        pltpu.make_async_copy(done.at[:, columns], out.at[:, columns], sem).start()
    before = last_top[...], last_total[...], last_summed[...]
    _, total, summed = attend(queries_of(q_buf, heads - 1, group), last_kv[0], last_kv[1], last_bias[...], before)
    result = (summed / total).astype(jnp.bfloat16)
    for member in range(group):
        result_buf[:, member * HEAD_SIZE : (member + 1) * HEAD_SIZE] = result[member * rows : (member + 1) * rows]
    pltpu.make_async_copy(result_buf, out.at[:, pl.ds(rest, group * HEAD_SIZE)], sem).start()
    pltpu.make_async_copy(done, out, sem).wait()


def kernel(
    sizes, q_hbm, k_hbm, v_hbm, lengths_hbm,
    out_buf, q_buf, last_kv, last_bias, last_top, last_total, last_summed,
    held, stage, bias, top_buf, total_buf, summed_buf, lengths,
    q_sem, kv_sem, send_sem, far_sem, recv_sem, stage_sem, lengths_sem,
):
    tp_count, dp_count, sp_count, hops, heads, group = sizes
    rows = q_hbm.shape[0]
    lines = dp_count * sp_count
    blocks = tp_count * lines
    line, core, plane = (lax.axis_index(axis) for axis in ("sp", "dp", "tp"))
    me = (plane * dp_count + core) * sp_count + line

    def device(index):
        index = lax.rem(index + 2 * blocks, blocks)
        return {"tp": index // lines, "dp": (index // sp_count) % dp_count, "sp": index % sp_count}

    far = sp_count - line
    is_far = (far <= hops) & (me + far < blocks)
    crosses = core == dp_count - 1
    odd = lax.rem(far, 2) == 1
    turns = is_far & crosses & odd
    goes_far = is_far & jnp.logical_not(turns)
    relays = (far <= hops) & crosses & odd & (plane >= 1)
    to_right = line < sp_count - 1
    right, left, turn, turned = device(me + 1), device(me - 1), device(me + lines), device(me - lines)
    far_target = device(me + far - jnp.where(relays, lines, 0))

    def far_sender(target, distance):
        return device(target - distance + (jnp.where(core == 0, lines, 0) if distance % 2 == 1 else 0))

    def load(head, which):
        source = (k_hbm, v_hbm)[which]
        return pltpu.make_async_copy(
            source.at[:, pl.ds(head * HEAD_SIZE, HEAD_SIZE)], held.at[0, 2 * head + which], kv_sem.at[head]
        )

    get_q = pltpu.make_async_copy(q_hbm, q_buf, q_sem)

    def copy(source, target, send, receive, where):
        return pltpu.make_async_remote_copy(
            src_ref=source, dst_ref=target, send_sem=send, recv_sem=receive, device_id=where, device_id_type=MESH
        )

    pieces = [pl.ds(2 * head, 2) for head in range(heads)]

    def forward(slot, n):
        rows_of = pieces[n]
        return copy(
            held.at[slot, rows_of], held.at[slot + 1, rows_of], send_sem, recv_sem.at[slot, n], right
        )

    def send_far(n):
        rows_of = pieces[n]
        return copy(held.at[0, rows_of], held.at[far, rows_of], far_sem, recv_sem.at[far - 1, n], far_target)

    def send_turn(n):
        rows_of = pieces[n]
        return copy(held.at[0, rows_of], stage.at[rows_of], far_sem, stage_sem.at[n], turn)

    def send_relay(n):
        rows_of = pieces[n]
        return copy(stage.at[rows_of], held.at[far, rows_of], far_sem, recv_sem.at[far - 1, n], far_target)

    def receive(slot, n):
        pl.when(me >= slot)(forward(slot - 1, n).wait_recv)
        if slot < hops:
            pl.when(to_right & (me >= slot))(forward(slot, n).start)

    barrier = pltpu.get_barrier_semaphore()

    def greet(condition, where):
        @pl.when(condition)
        def _():
            pl.semaphore_signal(barrier, inc=1, device_id=where, device_id_type=MESH)

    greet(line >= 1, left)
    for distance in range(1, hops + 1):
        greet((line == 0) & (me >= distance), far_sender(me, distance))
    greet(relays, turned)
    get_lengths = pltpu.make_async_copy(lengths_hbm, lengths, lengths_sem)
    for head in range(heads):
        for which in range(2):
            load(head, which).start()
    peers = sum(condition.astype(jnp.int32) for condition in (to_right, goes_far, relays, turns))

    @pl.when(peers > 0)
    def _():
        pl.semaphore_wait(barrier, peers)

    def start_far(condition, start, stop):
        @pl.when(goes_far & to_right & condition)
        def _():
            for n in range(start, stop):
                send_far(n).start()

    for n in range(heads):
        both = held.at[0, pl.ds(2 * n, 2)]
        pltpu.make_async_copy(both, both, kv_sem.at[n]).wait()
        if n == 0:
            start_far(True, 0, 1)
        pl.when(to_right)(forward(0, n).start)
        pl.when(turns)(send_turn(n).start)
        pl.when(goes_far & jnp.logical_not(to_right) & (True if n < heads - 1 else plane == 0))(send_far(n).start)
    start_far(jnp.logical_not(crosses), 1, heads)
    get_lengths.start()
    get_q.start()
    for slot in range(1, hops + 1):

        @pl.when(me < slot)
        def _():
            held[slot] = jnp.zeros_like(held[slot])

    get_lengths.wait()
    base = me * rows
    row = lax.broadcasted_iota(jnp.int32, (rows, rows), 0)
    column = lax.broadcasted_iota(jnp.int32, (rows, rows), 1)
    first = jnp.zeros((rows, rows), jnp.int32)
    end = jnp.int32(0)
    for entry in range(lengths.shape[0]):
        end = end + lengths[entry]
        first = jnp.where(base + row >= end, end, first)
    bias[0] = jnp.where((column <= row) & (base + column >= first), 0.0, DEAD)
    for slot in range(1, hops + 1):
        bias[slot] = jnp.where(base - slot * rows + column >= first, 0.0, DEAD)

    last_bias[...] = bias[hops]
    get_q.wait()
    for step in range(hops + 1):
        for head in range(heads):
            if step > 0:
                if step == 1 and head == 0:

                    @pl.when(relays)
                    def _():
                        for n in range(heads):
                            send_turn(n).wait_recv()
                            send_relay(n).start()

                receive(step, head)
            if step == hops and head == heads - 1:
                last_kv[...] = held[hops, pl.ds(2 * head, 2)]
                break
            final = head == heads - 1
            tops, totals, sums = (
                (last_top, last_total, last_summed) if final
                else (top_buf.at[head], total_buf.at[head], summed_buf.at[head])
            )
            before = None if step == 0 else (tops[...], totals[...], sums[...])
            top, total, summed = attend(
                queries_of(q_buf, head, group), held[step, 2 * head], held[step, 2 * head + 1], bias[step], before
            )
            if step < hops:
                tops[...], totals[...], sums[...] = top, total, summed
            else:
                result = (summed / total).astype(jnp.bfloat16)
                for member in range(group):
                    a = (head * group + member) * HEAD_SIZE
                    out_buf[:, a : a + HEAD_SIZE] = result[member * rows : (member + 1) * rows]
            if step == 0 and head == heads - 1:
                pl.when(goes_far & jnp.logical_not(to_right) & (plane > 0))(send_far(heads - 1).start)
            if step == 1 and head == heads - 1:
                start_far(crosses, 1, heads)

    def wait_sent(condition, count, sem):
        for slots in range(1, hops + 1):

            @pl.when(condition & (count == slots))
            def _():
                sent = held.at[pl.ds(0, slots)]
                pltpu.make_async_copy(sent, sent, sem).wait()

    wait_sent(to_right, jnp.minimum(me + 1, hops), send_sem)
    wait_sent(goes_far | turns | relays, (goes_far | turns).astype(jnp.int32) + relays.astype(jnp.int32), far_sem)


def solution(mesh):
    tp_count, dp_count, sp_count = (mesh.shape[axis] for axis in ("tp", "dp", "sp"))
    hops = max(sp_count // 2, 1)

    def local(queries, keys, values, doc_lengths):
        rows, width = queries.shape
        heads = keys.shape[1] // HEAD_SIZE
        group = width // keys.shape[1]
        sizes = (tp_count, dp_count, sp_count, hops, heads, group)
        hbm = pl.BlockSpec(memory_space=pltpu.HBM)
        arguments = (queries, keys, values, doc_lengths)
        vmem = pl.BlockSpec(memory_space=pltpu.VMEM)
        state = pltpu.VMEM((group * rows, HEAD_SIZE), jnp.float32)
        passed = [
            pltpu.VMEM((rows, width), jnp.bfloat16),
            pltpu.VMEM((rows, width), jnp.bfloat16),
            pltpu.VMEM((2, rows, HEAD_SIZE), jnp.bfloat16),
            pltpu.VMEM((rows, rows), jnp.float32),
            state, state, state,
        ]
        states = pltpu.VMEM((heads - 1, group * rows, HEAD_SIZE), jnp.float32)
        parts = pl.pallas_call(
            functools.partial(kernel, sizes),
            out_shape=[jax.ShapeDtypeStruct(x.shape, x.dtype) for x in passed],
            in_specs=[hbm] * 4,
            out_specs=[vmem] * len(passed),
            scratch_shapes=[
                pltpu.VMEM((hops + 1, 2 * heads, rows, HEAD_SIZE), jnp.bfloat16),
                pltpu.VMEM((2 * heads, rows, HEAD_SIZE), jnp.bfloat16),
                pltpu.VMEM((hops + 1, rows, rows), jnp.float32),
                states, states, states,
                pltpu.SMEM(doc_lengths.shape, jnp.int32),
                pltpu.SemaphoreType.DMA,
                pltpu.SemaphoreType.DMA((heads,)),
                pltpu.SemaphoreType.DMA,
                pltpu.SemaphoreType.DMA,
                pltpu.SemaphoreType.DMA((hops, heads)),
                pltpu.SemaphoreType.DMA((heads,)),
                pltpu.SemaphoreType.DMA,
            ],
            compiler_params=pltpu.CompilerParams(collective_id=0, has_side_effects=True, vmem_limit_bytes=32 << 20),
        )(*(pltpu.with_memory_space_constraint(x, pltpu.HBM) for x in arguments))
        return pl.pallas_call(
            functools.partial(finish, heads, group),
            out_shape=jax.ShapeDtypeStruct((rows, width), jnp.bfloat16),
            in_specs=[vmem] * len(passed),
            out_specs=hbm,
            scratch_shapes=[pltpu.VMEM((rows, group * HEAD_SIZE), jnp.bfloat16), pltpu.SemaphoreType.DMA],
            compiler_params=pltpu.CompilerParams(vmem_limit_bytes=16 << 20),
        )(*parts)

    spec = P(("groups", "tp", "dp", "sp"), None)
    return jax.shard_map(
        local, mesh=mesh, in_specs=(spec, spec, spec, P("groups")), out_specs=spec, check_vma=False
    )
```

```python
import functools
import math

import jax
import jax.numpy as jnp
from jax import lax
from jax.experimental import pallas as pl
from jax.experimental.pallas import tpu as pltpu
from jax.sharding import PartitionSpec as P

HEAD_SIZE = 128
MESH = pl.DeviceIdType.MESH
DEAD = -1e30


def queries_of(q_buf, head, group):
    columns = [(head * group + member) * HEAD_SIZE for member in range(group)]
    return jnp.concatenate([q_buf[:, a : a + HEAD_SIZE] for a in columns], axis=0)


def weigh(queries, keys, bias, before):
    rows = keys.shape[0]
    factor = HEAD_SIZE ** (-0.5) * math.log2(math.e)
    score = lax.dot_general(queries, keys, (((1,), (1,)), ((), ())), preferred_element_type=jnp.float32)
    score = (score.reshape(-1, rows, rows) + bias).reshape(-1, rows)
    top, fade = jnp.max(score, axis=1, keepdims=True), None
    if before is not None:
        top = jnp.maximum(top, before[0])
        fade = jnp.exp2((before[0] - top) * factor)
    weight = jnp.exp2((score - top) * factor)
    total = jnp.sum(weight, axis=1, keepdims=True)
    if before is not None:
        total = total + before[1] * fade
    return weight.astype(jnp.bfloat16), top, total, fade


def finish(heads, group, done, last_values, last_weight, last_scale, last_kept, out, result_buf, sem):
    rows = last_values.shape[1]
    width = group * HEAD_SIZE
    for head in range(heads - 2):
        columns = pl.ds(head * width, width)
        pltpu.make_async_copy(done.at[:, columns], out.at[:, columns], sem).start()
    for other in range(2):
        summed = jnp.dot(last_weight[other], last_values[other], preferred_element_type=jnp.float32)
        result = (summed * last_scale[other] + last_kept[other]).astype(jnp.bfloat16)
        for member in range(group):
            a = other * width + member * HEAD_SIZE
            result_buf[:, a : a + HEAD_SIZE] = result[member * rows : (member + 1) * rows]
        pltpu.make_async_copy(
            result_buf.at[:, pl.ds(other * width, width)], out.at[:, pl.ds((heads - 2 + other) * width, width)], sem
        ).start()
    pltpu.make_async_copy(done, out, sem).wait()


def kernel(
    sizes, q_hbm, k_hbm, v_hbm, lengths_hbm,
    out_buf, last_values, last_weight, last_scale, last_kept, q_buf,
    held, stage, bias, top_buf, total_buf, summed_buf, lengths,
    q_sem, kv_sem, send_sem, far_sem, recv_sem, stage_sem, lengths_sem,
):
    tp_count, dp_count, sp_count, hops, heads, group = sizes
    rows = q_hbm.shape[0]
    lines = dp_count * sp_count
    blocks = tp_count * lines
    line, core, plane = (lax.axis_index(axis) for axis in ("sp", "dp", "tp"))
    me = (plane * dp_count + core) * sp_count + line

    def device(index):
        index = lax.rem(index + 2 * blocks, blocks)
        return {"tp": index // lines, "dp": (index // sp_count) % dp_count, "sp": index % sp_count}

    far = sp_count - line
    is_far = (far <= hops) & (me + far < blocks)
    crosses = core == dp_count - 1
    odd = lax.rem(far, 2) == 1
    turns = is_far & crosses & odd
    goes_far = is_far & jnp.logical_not(turns)
    relays = (far <= hops) & crosses & odd & (plane >= 1)
    to_right = line < sp_count - 1
    right, left, turn, turned = device(me + 1), device(me - 1), device(me + lines), device(me - lines)
    far_target = device(me + far - jnp.where(relays, lines, 0))

    def far_sender(target, distance):
        return device(target - distance + (jnp.where(core == 0, lines, 0) if distance % 2 == 1 else 0))

    split = heads - 2
    row_of = [2 * head if head < split else split + head for head in range(heads)], [
        2 * head + 1 if head < split else split + 2 + head for head in range(heads)
    ]

    def load(head, which):
        source, at = (k_hbm, v_hbm)[which], row_of[which][head]
        return pltpu.make_async_copy(
            source.at[:, pl.ds(head * HEAD_SIZE, HEAD_SIZE)], held.at[0, at], kv_sem.at[at // 2]
        )

    get_q = pltpu.make_async_copy(q_hbm, q_buf, q_sem)

    def copy(source, target, send, receive, where):
        return pltpu.make_async_remote_copy(
            src_ref=source, dst_ref=target, send_sem=send, recv_sem=receive, device_id=where, device_id_type=MESH
        )

    pieces = [pl.ds(2 * n, 2) for n in range(heads)]

    def forward(slot, n):
        rows_of = pieces[n]
        return copy(
            held.at[slot, rows_of], held.at[slot + 1, rows_of], send_sem, recv_sem.at[slot, n], right
        )

    def send_far(n):
        rows_of = pieces[n]
        return copy(held.at[0, rows_of], held.at[far, rows_of], far_sem, recv_sem.at[far - 1, n], far_target)

    def send_turn(n):
        rows_of = pieces[n]
        return copy(held.at[0, rows_of], stage.at[rows_of], far_sem, stage_sem.at[n], turn)

    def send_relay(n):
        rows_of = pieces[n]
        return copy(stage.at[rows_of], held.at[far, rows_of], far_sem, recv_sem.at[far - 1, n], far_target)

    def receive(slot, n):
        pl.when(me >= slot)(forward(slot - 1, n).wait_recv)
        if slot < hops:
            pl.when(to_right & (me >= slot))(forward(slot, n).start)

    barrier = pltpu.get_barrier_semaphore()

    def greet(condition, where):
        @pl.when(condition)
        def _():
            pl.semaphore_signal(barrier, inc=1, device_id=where, device_id_type=MESH)

    greet(line >= 1, left)
    for distance in range(1, hops + 1):
        greet((line == 0) & (me >= distance), far_sender(me, distance))
    greet(relays, turned)
    get_lengths = pltpu.make_async_copy(lengths_hbm, lengths, lengths_sem)
    for head in range(heads):
        for which in range(2):
            load(head, which).start()
    peers = sum(condition.astype(jnp.int32) for condition in (to_right, goes_far, relays, turns))

    @pl.when(peers > 0)
    def _():
        pl.semaphore_wait(barrier, peers)

    def start_far(condition, start, stop):
        @pl.when(goes_far & to_right & condition)
        def _():
            for n in range(start, stop):
                send_far(n).start()

    for n in range(heads):
        both = held.at[0, pieces[n]]
        pltpu.make_async_copy(both, both, kv_sem.at[n]).wait()
        if n < 2:
            start_far(crosses | (n == 0), n, n + 1)
        pl.when(to_right)(forward(0, n).start)
        pl.when(turns)(send_turn(n).start)
        pl.when(goes_far & jnp.logical_not(to_right) & (True if n < heads - 1 else plane == 0))(send_far(n).start)
    start_far(jnp.logical_not(crosses), 1, heads)
    get_lengths.start()
    get_q.start()
    for slot in range(1, hops + 1):

        @pl.when(me < slot)
        def _():
            held[slot] = jnp.zeros_like(held[slot])

    get_lengths.wait()
    base = me * rows
    row = lax.broadcasted_iota(jnp.int32, (rows, rows), 0)
    column = lax.broadcasted_iota(jnp.int32, (rows, rows), 1)
    first = jnp.zeros((rows, rows), jnp.int32)
    end = jnp.int32(0)
    for entry in range(lengths.shape[0]):
        end = end + lengths[entry]
        first = jnp.where(base + row >= end, end, first)
    bias[0] = jnp.where((column <= row) & (base + column >= first), 0.0, DEAD)
    for slot in range(1, hops + 1):
        bias[slot] = jnp.where(base - slot * rows + column >= first, 0.0, DEAD)

    def weigh_at(step, head):
        before = None if step == 0 else (top_buf[head], total_buf[head])
        return weigh(queries_of(q_buf, head, group), held[step, row_of[0][head]], bias[step], before)

    get_q.wait()
    for step in range(hops + 1):
        for head in range(split + 1):
            if step > 0:
                if step == 1 and head == 0:

                    @pl.when(relays)
                    def _():
                        for n in range(heads):
                            send_turn(n).wait_recv()
                            send_relay(n).start()

                receive(step, head)
            if step == 1 and head == 0:
                pl.when(goes_far & jnp.logical_not(to_right) & (plane > 0))(send_far(heads - 1).start)
            weighed = [weigh_at(step, at) for at in ((head,) if head < split else (split, split + 1))]
            if step == 1 and head == split:
                start_far(crosses, 2, heads)
            if head == split and step == hops:
                for other, (weight, top, total, fade) in enumerate(weighed):
                    scale = jnp.broadcast_to(1.0 / total, last_scale.shape[1:])
                    last_weight[other], last_scale[other] = weight, scale
                    last_kept[other] = summed_buf[split + other] * (fade * scale)
            if head == split and step > 0:
                receive(step, split + 1)
            if head == split and step == hops:
                last_values[...] = held[hops, pl.ds(row_of[1][split], 2)]
                continue
            for at, (weight, top, total, fade) in enumerate(weighed, head):
                summed = jnp.dot(weight, held[step, row_of[1][at]], preferred_element_type=jnp.float32)
                if step > 0:
                    summed = summed + summed_buf[at] * fade
                if step < hops:
                    top_buf[at], total_buf[at] = (jnp.broadcast_to(x, summed.shape) for x in (top, total))
                    summed_buf[at] = summed
                else:
                    result = (summed / total).astype(jnp.bfloat16)
                    for member in range(group):
                        a = (at * group + member) * HEAD_SIZE
                        out_buf[:, a : a + HEAD_SIZE] = result[member * rows : (member + 1) * rows]

    def wait_sent(condition, count, sem):
        for slots in range(1, hops + 1):

            @pl.when(condition & (count == slots))
            def _():
                sent = held.at[pl.ds(0, slots)]
                pltpu.make_async_copy(sent, sent, sem).wait()

    wait_sent(to_right, jnp.minimum(me + 1, hops), send_sem)
    wait_sent(goes_far | turns | relays, (goes_far | turns).astype(jnp.int32) + relays.astype(jnp.int32), far_sem)


def solution(mesh):
    tp_count, dp_count, sp_count = (mesh.shape[axis] for axis in ("tp", "dp", "sp"))
    hops = max(sp_count // 2, 1)

    def local(queries, keys, values, doc_lengths):
        rows, width = queries.shape
        heads = keys.shape[1] // HEAD_SIZE
        group = width // keys.shape[1]
        sizes = (tp_count, dp_count, sp_count, hops, heads, group)
        hbm = pl.BlockSpec(memory_space=pltpu.HBM)
        arguments = (queries, keys, values, doc_lengths)
        vmem = pl.BlockSpec(memory_space=pltpu.VMEM)
        state = pltpu.VMEM((2, group * rows, HEAD_SIZE), jnp.float32)
        passed = [
            pltpu.VMEM((rows, width), jnp.bfloat16),
            pltpu.VMEM((2, rows, HEAD_SIZE), jnp.bfloat16),
            pltpu.VMEM((2, group * rows, rows), jnp.bfloat16),
            state, state,
        ]
        states = pltpu.VMEM((heads, group * rows, HEAD_SIZE), jnp.float32)
        parts = pl.pallas_call(
            functools.partial(kernel, sizes),
            out_shape=[jax.ShapeDtypeStruct(x.shape, x.dtype) for x in passed],
            in_specs=[hbm] * 4,
            out_specs=[vmem] * len(passed),
            scratch_shapes=[
                pltpu.VMEM((rows, width), jnp.bfloat16),
                pltpu.VMEM((hops + 1, 2 * heads, rows, HEAD_SIZE), jnp.bfloat16),
                pltpu.VMEM((2 * heads, rows, HEAD_SIZE), jnp.bfloat16),
                pltpu.VMEM((hops + 1, rows, rows), jnp.float32),
                states, states, states,
                pltpu.SMEM(doc_lengths.shape, jnp.int32),
                pltpu.SemaphoreType.DMA,
                pltpu.SemaphoreType.DMA((heads,)),
                pltpu.SemaphoreType.DMA,
                pltpu.SemaphoreType.DMA,
                pltpu.SemaphoreType.DMA((hops, heads)),
                pltpu.SemaphoreType.DMA((heads,)),
                pltpu.SemaphoreType.DMA,
            ],
            compiler_params=pltpu.CompilerParams(collective_id=0, has_side_effects=True, vmem_limit_bytes=32 << 20),
        )(*(pltpu.with_memory_space_constraint(x, pltpu.HBM) for x in arguments))
        return pl.pallas_call(
            functools.partial(finish, heads, group),
            out_shape=jax.ShapeDtypeStruct((rows, width), jnp.bfloat16),
            in_specs=[vmem] * len(passed),
            out_specs=hbm,
            scratch_shapes=[pltpu.VMEM((rows, 2 * group * HEAD_SIZE), jnp.bfloat16), pltpu.SemaphoreType.DMA],
            compiler_params=pltpu.CompilerParams(vmem_limit_bytes=16 << 20),
        )(*parts)

    spec = P(("groups", "tp", "dp", "sp"), None)
    return jax.shard_map(
        local, mesh=mesh, in_specs=(spec, spec, spec, P("groups")), out_specs=spec, check_vma=False
    )
```
